32 devices in a mesh: expert: 4 (over z), mp: 8 (over y, x, core).
Axes of the slice: x: 2, y: 2, z: 4, core: 2. Of those that a mesh axis runs over, the one named last changes fastest.
Arguments:
- tokens: bfloat16 [512, 4096], P(('expert', 'mp')), may hold values from -6 to 6
- gain: bfloat16 [4096], replicated, may hold values from 0.5 to 1.5
- expert_ids: int32 [512, 2], P(('expert', 'mp')), may hold values from 0 to 3, all different within a row; in each aligned block of 16 rows (0 to 15, 16 to 31, ...) at most 10 rows name the same one
- gate_num: int32 [512], P(('expert', 'mp')), may hold values from 1 to 1023
- w_gate: bfloat16 [4, 4096, 14336], P('expert', None, 'mp'), may hold values from -0.09375 to 0.09375
- w_up: bfloat16 [4, 4096, 14336], P('expert', None, 'mp'), may hold values from -0.09375 to 0.09375
- w_down: bfloat16 [4, 14336, 4096], P('expert', 'mp'), may hold values from -0.046875 to 0.046875
Outputs:
- mixed_out: bfloat16 [512, 4096], P(('expert', 'mp'))
The draws below stay inside these ranges and needn't reach their ends.
Inputs may be any that keep to these rules, and one draw needn't show every extreme that they name: `expert_ids`: the 2 ids of a token differ. Within the rows of one device no expert is named more than 10 times, and some expert reaches 10 on some devices.
All inputs are finite; a program needn't handle non-finite values.
Results may differ from the reference program's by a relative error of at most 0.019.
Values may be sent and summed in bfloat16 or wider, within the bound.
A program may use at most 128 MiB of HBM per device.

```python
import math
import jax
import jax.numpy as jnp
import numpy as np
from jax import lax

D = 4096
FF = 14336
TOP = 2
DENOM = 1024
TOK_DEV = 16
EXPERTS = 4
TOKENS = 512
CAP = 10
ROWS_MAX = 320
FF_SHARD = 1792
N_MP = 8


def plant(values, rng, low, high):
    extent = values.shape
    index_at = [jax.random.randint(jax.random.fold_in(rng, axis), (), 0, extent[axis]) for axis in range(len(extent))]
    values = values.at[tuple(index_at)].set(low)
    longest = extent.index(max(extent))
    index_at[longest] = (index_at[longest] + 1) % extent[longest]
    return values.at[tuple(index_at)].set(high)


def shard_levels(rng, shape, pieces, least, largest):
    loudness, own = 1.0, jax.random.fold_in(rng, 6)
    for position, blocks in pieces:
        steps = jnp.exp(jax.random.uniform(jax.random.fold_in(own, position), (blocks,), jnp.float32, least / len(pieces), largest / len(pieces)))
        loudness = loudness * jnp.repeat(steps, shape[position] // blocks).reshape([-1 if axis == position else 1 for axis in range(len(shape))])
    return loudness


def assign_block(own_key, own, number, rows, count, top, most, lean):
    order = jax.random.permutation(own_key, count)
    heavy_load, common = shares(count, rows * top, most, lean, True), shares(count, rows * top, most, lean, False)
    places = jnp.arange(count)

    def named(lengths, rotation):
        used = int((lengths > 0).sum())
        fixed = max(1, used // 4)
        moved = fixed + (places - fixed + rotation * (used - fixed)) % max(1, count - fixed)
        return jnp.zeros((count,), jnp.int32).at[order[jnp.where(places < fixed, places, moved)]].set(jnp.asarray(lengths, jnp.int32))

    lengths = jnp.where(number % 4 == 0, named(heavy_load, number // 4), named(common, number - number // 4 - 1))
    mixed = jax.random.permutation(jax.random.fold_in(own, 3), count)
    source_of, taker = mixed[0:count // 2 * 2:2], mixed[1:count // 2 * 2:2]
    margin = jnp.minimum(lengths[source_of] - 1, most - lengths[taker]) // 2
    margin = jnp.where((source_of == order[0]) | (taker == order[0]) | (lengths[taker] == 0), 0, jnp.maximum(margin, 0))
    moved = jax.random.randint(jax.random.fold_in(own, 4), (count // 2,), 0, 1 << 20) % (margin + 1)
    lengths = lengths.at[source_of].add(-moved).at[taker].add(moved)
    labels = jnp.searchsorted(jnp.cumsum(lengths), jnp.arange(rows * top), side="right").astype(jnp.int32)
    grid = labels.reshape(top, rows).T
    grid = grid[jax.random.permutation(jax.random.fold_in(own, 1), rows)]
    rotation = jax.random.randint(jax.random.fold_in(own, 2), (rows, 1), 0, top)
    return jnp.take_along_axis(grid, (jnp.arange(top)[None, :] + rotation) % top, axis=1)


def shares(number_of, total, reach, skew, full):
    portions = [(1 << 20) // math.isqrt(grade ** skew) + 1 for grade in range(1, number_of + 1)]
    largest = reach if full else min(reach, max(-(-total // number_of), total * portions[0] // sum(portions)))
    least = 1 if total - largest >= number_of - 1 else 0
    counts, spare = [largest] + [least] * (number_of - 1), total - largest - least * (number_of - 1)
    while spare > 0:
        candidates = [i for i in range(1, number_of) if counts[i] < largest] or [i for i in range(1, number_of) if counts[i] < reach]
        whole, budget = sum([portions[i] for i in candidates]), spare
        for i in candidates:
            extra = min(reach - counts[i], max(1, budget * portions[i] // whole), spare)
            counts[i] = counts[i] + extra
            spare = spare - extra
    return np.array(counts)


def bell_draw(stream_key, shape, spread, most, shards=(), kind=jnp.bfloat16):
    values = jax.random.normal(stream_key, shape, jnp.float32) * spread
    if len(shards) > 0:
        values = shard_levels(stream_key, shape, shards, -0.22, 0.18) * values
    return jnp.clip(values, min=-most, max=most).astype(kind)


def setup_inputs(seed: int = 0) -> dict:
    keys = jax.random.split(jax.random.key(seed), 8)
    tokens = bell_draw(keys[0], (TOKENS, D), 1.0, 6.0, ((0, 32),))
    gain = jnp.clip(1.0 + 0.1 * jax.random.normal(keys[1], (D,), jnp.float32), 0.5, 1.5).astype(jnp.bfloat16)
    expert_ids_keys = jax.random.split(jax.random.fold_in(keys[2], 1), TOKENS // TOK_DEV)
    expert_ids_turns = jax.random.permutation(jax.random.fold_in(keys[2], 3), TOKENS // TOK_DEV)
    expert_ids = jax.vmap(lambda own, number: assign_block(jax.random.fold_in(keys[2], 2), own, number, TOK_DEV, EXPERTS, TOP, CAP, 2))(expert_ids_keys, expert_ids_turns).reshape((TOKENS, TOP))
    gate_num = plant(jax.random.randint(keys[3], (TOKENS,), 1, DENOM), jax.random.fold_in(keys[3], 1), 1, DENOM - 1).astype(jnp.int32)
    w_gate = bell_draw(keys[4], (EXPERTS, D, FF), D ** -0.5, 0.09375, ((0, 4), (2, 8)))
    w_up = bell_draw(keys[5], (EXPERTS, D, FF), D ** -0.5, 0.09375, ((0, 4), (2, 8)))
    w_down = bell_draw(keys[6], (EXPERTS, FF, D), FF ** -0.5, 0.046875, ((0, 4), (1, 8)))
    return dict(tokens=tokens, gain=gain, expert_ids=expert_ids, gate_num=gate_num, w_gate=w_gate, w_up=w_up, w_down=w_down)


def rms_normed(tokens, gain):
    values = tokens.astype(jnp.float32)
    inverse = lax.rsqrt(lax.optimization_barrier(jnp.mean(values * values, axis=1, keepdims=True)) + 1e-05)
    return (values * inverse * gain.astype(jnp.float32)).astype(jnp.bfloat16)

def swiglu(row_block, gate_matrix, up_matrix):
    gate_proj = jnp.dot(row_block, gate_matrix, preferred_element_type=jnp.float32)
    up_proj = jnp.dot(row_block, up_matrix, preferred_element_type=jnp.float32)
    return (jax.nn.silu(gate_proj) * up_proj).astype(jnp.bfloat16)

def reference(tokens, gain, expert_ids, gate_num, w_gate, w_up, w_down):
    normed = rms_normed(tokens, gain)
    flat_ids = expert_ids.reshape(-1).astype(jnp.int32)
    first_share = gate_num.astype(jnp.float32) / DENOM
    weights = jnp.stack([first_share, 1.0 - first_share], axis=1).reshape(-1)

    def one_expert(expert):
        off_expert = (flat_ids != expert).astype(jnp.int32)
        slot_order = jnp.argsort(off_expert, stable=True)[:ROWS_MAX].astype(jnp.int32)
        filled = flat_ids[slot_order] == expert
        token_rows = (slot_order // TOP).astype(jnp.int32)
        row_block = jnp.take(normed, token_rows, axis=0)
        row_block = jnp.where(filled[:, None], row_block, jnp.zeros_like(row_block))
        hidden = swiglu(row_block, w_gate[expert], w_up[expert])
        hidden_groups = hidden.reshape(ROWS_MAX, N_MP, FF_SHARD).transpose(1, 0, 2)
        down_rows = w_down[expert].reshape(N_MP, FF_SHARD, D)

        def add_group(running, group_pair):
            group_part = jnp.dot(group_pair[0], group_pair[1], preferred_element_type=jnp.float32).astype(jnp.bfloat16)
            group_part = lax.optimization_barrier(group_part)
            return (running + group_part.astype(jnp.float32), None)
        running, _ = lax.scan(add_group, jnp.zeros((ROWS_MAX, D), jnp.float32), (hidden_groups, down_rows))
        result = lax.optimization_barrier(running.astype(jnp.bfloat16)).astype(jnp.float32)
        slot_weight = jnp.where(filled, weights[slot_order], jnp.float32(0.0))
        return (result * slot_weight[:, None], token_rows)
    scaled, token_index = lax.map(one_expert, jnp.arange(EXPERTS, dtype=jnp.int32))
    mixed_out = jnp.zeros((TOKENS, D), jnp.float32).at[token_index.reshape(-1)].add(scaled.reshape(-1, D))
    return mixed_out.astype(jnp.bfloat16)
```

```python
import functools

import jax
import jax.numpy as jnp
from jax import lax
from jax.experimental import pallas as pl
from jax.experimental.pallas import tpu as pltpu
from jax.sharding import PartitionSpec as P

DENOM = 1024


def rms_normed(tokens, gain):
    values = tokens.astype(jnp.float32)
    inverse = lax.rsqrt(jnp.mean(values * values, axis=1, keepdims=True) + 1e-05)
    return (values * inverse * gain.astype(jnp.float32)).astype(jnp.bfloat16)


def swiglu(row_block, gate_matrix, up_matrix):
    gate_proj = jnp.dot(row_block, gate_matrix, preferred_element_type=jnp.float32)
    up_proj = jnp.dot(row_block, up_matrix, preferred_element_type=jnp.float32)
    return (jax.nn.silu(gate_proj) * up_proj).astype(jnp.bfloat16)


def slot_plan(expert_ids, experts, capacity):
    flat_ids = expert_ids.reshape(-1)
    slot_count = flat_ids.shape[0]
    slot_order = jnp.arange(slot_count, dtype=jnp.int32)
    earlier = (flat_ids[:, None] == flat_ids[None, :]) & (slot_order[None, :] < slot_order[:, None])
    position = jnp.sum(earlier.astype(jnp.int32), axis=1)
    target = flat_ids * capacity + position
    slot_ids = jnp.arange(experts * capacity, dtype=jnp.int32)
    matched = target[None, :] == slot_ids[:, None]
    token_of = slot_order[None, :] // expert_ids.shape[1] + 1
    slot_owner = jnp.sum(jnp.where(matched, token_of, 0), axis=1) - 1
    return (target, slot_owner)


def body(tokens, gain, expert_ids, gate_num, w_gate, w_up, w_down):
    groups = lax.axis_size("expert")
    tok_rows, model_width = tokens.shape
    top_count = expert_ids.shape[1]
    capacity = (5 * tok_rows * top_count + 4 * groups - 1) // (4 * groups)
    normed = rms_normed(tokens, gain)
    target, slot_owner = slot_plan(expert_ids, groups, capacity)
    gate_matrix = w_gate[0]
    up_matrix = w_up[0]
    down_matrix = w_down[0]
    picked = jnp.take(normed, jnp.maximum(slot_owner, 0), axis=0)
    outgoing = jnp.where((slot_owner >= 0)[:, None], picked, jnp.zeros_like(picked))
    received = lax.all_to_all(
        outgoing.reshape(groups, capacity, model_width),
        "expert",
        split_axis=0,
        concat_axis=0,
        tiled=True,
    )
    received = received.reshape(groups * capacity, model_width)
    hidden = swiglu(lax.all_gather(received, "mp", axis=0, tiled=True), gate_matrix, up_matrix)
    summed = lax.psum_scatter(
        jnp.dot(hidden, down_matrix, preferred_element_type=jnp.float32).astype(jnp.bfloat16),
        "mp",
        scatter_dimension=0,
        tiled=True,
    )
    outcome = summed.reshape(groups, capacity, model_width)
    returned = lax.all_to_all(outcome, "expert", split_axis=0, concat_axis=0, tiled=True)
    flat_back = returned.reshape(groups * capacity, model_width)
    chosen = (
        jnp.take(flat_back, target, axis=0)
        .astype(jnp.float32)
        .reshape(tok_rows, top_count, model_width)
    )
    first_share = gate_num.astype(jnp.float32) / DENOM
    mixed_out = (
        chosen[:, 0, :] * first_share[:, None] + chosen[:, 1, :] * (1.0 - first_share)[:, None]
    )
    return mixed_out.astype(jnp.bfloat16)


MESH = pl.DeviceIdType.MESH
F32, BF16 = jnp.float32, jnp.bfloat16


def fused_kernel(plan, tok, gain, meta, wg_hbm, wu_hbm, wd_hbm, out,
                 wg, wu, wd, xbuf, acc_g, acc_u, hidden, nbuf, norm_all, meta_all,
                 zsend, zrecv, psend, prcv, sums, r1, s2, r2, rsend, zret, mixbuf, orecv,
                 w_sem, wd_sem, n_sem, m_sem, ml_sem, z_ss, z_rs, x_ss, x_rs, y_ss, y_rs, f_ss, f_rs,
                 d_ss, d_rs, p_ss, p_rs, a_ss, a_rs, b_ss, b_rs, q_ss, q_rs, o_ss, o_rs):
    S, CW, groups, cap, stride, tile = plan
    toks, width = tok.shape
    half = width // 2
    rows = groups * cap
    ff = hidden.shape[1]
    myz = lax.axis_index("expert")
    mp = lax.axis_index("mp")
    core = mp % 2
    other = 1 - core
    k = mp // 2
    kx = k + 1 - 2 * (k % 2)
    ky = k + 2 - 4 * (k // 2)
    kd = 3 - k
    partner = {"mp": 2 * k + other}
    xn = {"mp": 2 * kx + core}
    yn = {"mp": 2 * ky + core}
    zs = [lax.rem(myz + d, groups) for d in range(groups)]

    def remote(src, dst, ss, rs, dev):
        return pltpu.make_async_remote_copy(src_ref=src, dst_ref=dst, send_sem=ss, recv_sem=rs,
                                            device_id=dev, device_id_type=MESH)

    barrier = pltpu.get_barrier_semaphore()
    peers = [partner, xn, yn] + [{"expert": zs[d]} for d in range(1, groups)]
    for dev in peers:
        pl.semaphore_signal(barrier, inc=1, device_id=dev, device_id_type=MESH)

    order = []
    for j in range(S):
        order += [core * S + j, other * S + j]

    def w_copies(c):
        at = pl.ds(pl.multiple_of(c * CW, CW), CW)
        return (pltpu.make_async_copy(wg_hbm.at[0, at, :], wg.at[at, :], w_sem.at[0, c]),
                pltpu.make_async_copy(wu_hbm.at[0, at, :], wu.at[at, :], w_sem.at[1, c]))

    def wd_copy(c):
        at = pl.ds(pl.multiple_of(c * CW, CW), CW)
        return pltpu.make_async_copy(wd_hbm.at[0, :, at], wd.at[:, at], wd_sem.at[c])

    meta_local = pltpu.make_async_copy(meta, meta_all.at[core], ml_sem)
    meta_local.start()
    for c in order:
        for copy in w_copies(c):
            copy.start()
    for j in range(S):
        wd_copy(other * S + j).start()
        wd_copy(core * S + j).start()

    values = tok[...].astype(F32)
    inverse = lax.rsqrt(jnp.mean(values * values, axis=1, keepdims=True) + 1e-05)
    normed = (values * inverse * gain[...].astype(F32)).astype(BF16)
    nbuf[0] = normed[:, :half]
    nbuf[1] = normed[:, half:]
    pl.semaphore_wait(barrier, len(peers))
    meta_copy = remote(meta, meta_all.at[core], m_sem.at[0], m_sem.at[1], partner)
    meta_copy.start()
    norm_copy = remote(nbuf.at[other], norm_all.at[core], n_sem.at[0], n_sem.at[1], partner)
    norm_copy.start()
    norm_all[core] = nbuf[core]

    meta_local.wait()
    meta_copy.wait_recv()
    info = meta_all[...].reshape(2 * toks, meta.shape[1])
    id0, id1, num = info[:, 0:1], info[:, 1:2], info[:, 2:3]
    lanes = lax.broadcasted_iota(jnp.int32, (2 * toks, 128), 1)
    oh0 = jnp.where(lanes == id0, 1.0, 0.0)
    oh1 = jnp.where(lanes == id1, 1.0, 0.0)
    tri_r = lax.broadcasted_iota(jnp.int32, (2 * toks, 2 * toks), 0)
    tri_c = lax.broadcasted_iota(jnp.int32, (2 * toks, 2 * toks), 1)
    tri = jnp.where(tri_c < tri_r, 1.0, 0.0).astype(BF16)
    cnt = jnp.dot(tri, (oh0 + oh1).astype(BF16), preferred_element_type=F32)
    lane_f = lanes.astype(F32)
    t0 = id0.astype(F32) * stride + jnp.sum(oh0 * cnt, axis=1, keepdims=True)
    t1 = id1.astype(F32) * stride + jnp.sum(oh1 * cnt, axis=1, keepdims=True)
    hit0, hit1 = lane_f == t0, lane_f == t1
    pick = jnp.where(hit0 | hit1, 1.0, 0.0)
    pick_t = jnp.transpose(pick).astype(BF16)
    low0 = num % 4
    low1 = (DENOM - num) % 4
    hi = jnp.where(hit0, (num - low0).astype(F32), jnp.where(hit1, (DENOM - num - low1).astype(F32), 0.0))
    lo = jnp.where(hit0, low0.astype(F32), jnp.where(hit1, low1.astype(F32), 0.0))
    mix = (jnp.concatenate([hi, lo], axis=0) * (1.0 / DENOM)).astype(BF16)

    norm_copy.wait_recv()

    def z_copy(j, d):
        return remote(zsend.at[j, zs[d]], zrecv.at[j, myz], z_ss.at[j, d], z_rs.at[j, d], {"expert": zs[d]})

    for j in range(S):
        block = norm_all[:, :, j * CW:(j + 1) * CW].reshape(2 * toks, CW)
        picked = jnp.dot(pick_t, block, preferred_element_type=F32).astype(BF16)
        for z in range(groups):
            zsend[j, z] = picked[z * stride:z * stride + cap]
        for d in range(1, groups):
            z_copy(j, d).start()
        zrecv[j, myz] = zsend[j, myz]

    acc_g[...] = jnp.zeros_like(acc_g)
    acc_u[...] = jnp.zeros_like(acc_u)

    def place(z):
        r = lax.broadcasted_iota(jnp.int32, (rows, cap), 0)
        c = lax.broadcasted_iota(jnp.int32, (rows, cap), 1)
        return jnp.where(r == c + z * cap, 1.0, 0.0).astype(BF16)

    def take(z):
        r = lax.broadcasted_iota(jnp.int32, (cap, rows), 0)
        c = lax.broadcasted_iota(jnp.int32, (cap, rows), 1)
        return jnp.where(c == r + z * cap, 1.0, 0.0).astype(BF16)

    def slot(j, who, core_of=core):
        return xbuf.at[core_of * S + j, who]

    def x_copy(j, who=None):
        return remote(slot(j, k), slot(j, k), x_ss.at[j], x_rs.at[j], xn)

    def y_copy(j):
        return remote(slot(j, k), slot(j, k), y_ss.at[j], y_rs.at[j], yn)

    def f_copy(j):
        if j % 2 == 0:
            return remote(slot(j, kx), slot(j, kx), f_ss.at[j], f_rs.at[j], yn)
        return remote(slot(j, ky), slot(j, ky), f_ss.at[j], f_rs.at[j], xn)

    whos = (k, kx, ky, kd)

    def d_copy(j, i):
        return remote(slot(j, whos[i]), slot(j, whos[i]), d_ss.at[j, i], d_rs.at[j, i], partner)

    def stage_c(j):
        total = jnp.zeros((rows, CW), F32)
        for d in range(1, groups):
            z_copy(j, d).wait_recv()
        for z in range(groups):
            total = total + jnp.dot(place(z), zrecv[j, z], preferred_element_type=F32)
        xbuf[core * S + j, k] = total.astype(BF16)
        x_copy(j).start()
        y_copy(j).start()
        d_copy(j, 0).start()

    def stage_d(j):
        x_copy(j).wait_recv()
        if j % 2 == 0:
            f_copy(j).start()
        d_copy(j, 1).start()
        y_copy(j).wait_recv()
        if j % 2 == 1:
            f_copy(j).start()
        d_copy(j, 2).start()

    def up_mm(c, last):
        for copy in w_copies(c):
            copy.wait()
        at = pl.ds(pl.multiple_of(c * CW, CW), CW)

        def step(n, carry):
            cols = pl.ds(pl.multiple_of(n * tile, tile), tile)
            x = xbuf[c].reshape(4 * rows, CW)
            g = acc_g[:, cols] + jnp.dot(x, wg[at, cols], preferred_element_type=F32)
            u = acc_u[:, cols] + jnp.dot(x, wu[at, cols], preferred_element_type=F32)
            if last:
                hidden[:, cols] = (g / (1.0 + jnp.exp(-g)) * u).astype(BF16)
            else:
                acc_g[:, cols] = g
                acc_u[:, cols] = u
            return carry

        lax.fori_loop(0, ff // tile, step, 0)

    def stage_e(j):
        f_copy(j).wait_recv()
        d_copy(j, 3).start()
        up_mm(core * S + j, False)
        for i in range(4):
            d_copy(j, i).wait_recv()
        up_mm(other * S + j, j == S - 1)

    ahead = max(1, S // 4)
    for j in range(S):
        stage_c(j)
    for j in range(S + ahead):
        if j < S:
            stage_d(j)
        if j >= ahead:
            stage_e(j - ahead)

    def down(c):
        at = pl.ds(pl.multiple_of(c * CW, CW), CW)
        wd_copy(c).wait()
        return jnp.dot(hidden[...], wd[:, at], preferred_element_type=F32)

    def p_copy(j):
        return remote(psend.at[j], prcv.at[j], p_ss.at[j], p_rs.at[j], partner)

    def near(j):
        return (kx, ky, xn, yn) if j % 2 == 0 else (ky, kx, yn, xn)

    def a_copy(j, i):
        first, _, dev, _ = near(j)
        return remote(sums.at[j, (first, kd)[i]], r1.at[j, i], a_ss.at[j, i], a_rs.at[j, i], dev)

    def b_copy(j):
        return remote(s2.at[j], r2.at[j], b_ss.at[j], b_rs.at[j], near(j)[3])

    def stage_0a(j):
        psend[j] = down(other * S + j).astype(BF16).reshape(4, rows, CW)
        p_copy(j).start()

    def stage_0(j):
        own = down(core * S + j).reshape(4, rows, CW)
        p_copy(j).wait_recv()
        sums[j] = (own + prcv[j].astype(F32)).astype(BF16)
        a_copy(j, 1).start()
        a_copy(j, 0).start()

    def stage_2(j):
        a_copy(j, 1).wait_recv()
        s2[j] = (sums[j, near(j)[1]].astype(F32) + r1[j, 1].astype(F32)).astype(BF16)
        b_copy(j).start()

    def q_copy(j, d):
        return remote(rsend.at[j, zs[d]], zret.at[j, myz], q_ss.at[j, d], q_rs.at[j, d], {"expert": zs[d]})

    def stage_3(j):
        a_copy(j, 0).wait_recv()
        b_copy(j).wait_recv()
        fin = (sums[j, k].astype(F32) + r1[j, 0].astype(F32) + r2[j].astype(F32)).astype(BF16)
        for z in range(groups):
            rsend[j, z] = jnp.dot(take(z), fin, preferred_element_type=F32).astype(BF16)
        for d in range(1, groups):
            q_copy(j, d).start()
        zret[j, myz] = rsend[j, myz]

    def o_copy(j):
        return remote(mixbuf.at[j, other], orecv.at[j], o_ss.at[j], o_rs.at[j], partner)

    def stage_4(j):
        for d in range(1, groups):
            q_copy(j, d).wait_recv()
        total = jnp.zeros((4 * toks, CW), F32)
        for z in range(groups):
            total = total + jnp.dot(mix[:, z * stride:z * stride + cap], zret[j, z], preferred_element_type=F32)
        mixed = (total[:2 * toks] + total[2 * toks:]).astype(BF16)
        mixbuf[j] = mixed.reshape(2, toks, CW)
        o_copy(j).start()
        out[:, pl.ds(pl.multiple_of((core * S + j) * CW, CW), CW)] = mixbuf[j, core]

    stage_0a(0)
    for j in range(S):
        if j + 1 < S:
            stage_0a(j + 1)
        stage_0(j)
    for j in range(S):
        stage_2(j)
    for j in range(S + 1):
        if j < S:
            stage_3(j)
        if j >= 1:
            stage_4(j - 1)
    for j in range(S):
        o_copy(j).wait_recv()
        out[:, pl.ds(pl.multiple_of((other * S + j) * CW, CW), CW)] = orecv[j]

    meta_copy.wait_send()
    norm_copy.wait_send()
    for j in range(S):
        for d in range(1, groups):
            z_copy(j, d).wait_send()
            q_copy(j, d).wait_send()
        for copy in (x_copy(j), y_copy(j), f_copy(j), p_copy(j), a_copy(j, 0), a_copy(j, 1), b_copy(j), o_copy(j)):
            copy.wait_send()
        for i in range(4):
            d_copy(j, i).wait_send()


def fused_body(tokens, gain, expert_ids, gate_num, w_gate, w_up, w_down):
    groups = lax.axis_size("expert")
    toks, width = tokens.shape
    ff = w_gate.shape[2]
    cap = 2 * ((5 * toks * expert_ids.shape[1] + 4 * groups - 1) // (4 * groups))
    stride = -(-cap // 16) * 16
    rows = groups * cap
    S = SPLIT
    CW = width // 2 // S
    meta = jnp.concatenate([expert_ids, gate_num[:, None]], axis=1)
    dma = pltpu.SemaphoreType.DMA
    vm = pltpu.VMEM
    scratch = [
        vm((width, ff), BF16), vm((width, ff), BF16), vm((ff, width), BF16),
        vm((2 * S, 4, rows, CW), BF16), vm((4 * rows, ff), F32), vm((4 * rows, ff), F32), vm((4 * rows, ff), BF16),
        vm((2, toks, width // 2), BF16), vm((2, toks, width // 2), BF16), vm((2, toks, 3), jnp.int32),
        vm((S, groups, cap, CW), BF16), vm((S, groups, cap, CW), BF16),
        vm((S, 4, rows, CW), BF16), vm((S, 4, rows, CW), BF16), vm((S, 4, rows, CW), BF16),
        vm((S, 2, rows, CW), BF16), vm((S, rows, CW), BF16), vm((S, rows, CW), BF16),
        vm((S, groups, cap, CW), BF16), vm((S, groups, cap, CW), BF16),
        vm((S, 2, toks, CW), BF16), vm((S, toks, CW), BF16),
        dma((2, 2 * S)), dma((2 * S,)), dma((2,)), dma((2,)), dma,
        dma((S, groups)), dma((S, groups)), dma((S,)), dma((S,)), dma((S,)), dma((S,)), dma((S,)), dma((S,)),
        dma((S, 4)), dma((S, 4)), dma((S,)), dma((S,)), dma((S, 2)), dma((S, 2)), dma((S,)), dma((S,)),
        dma((S, groups)), dma((S, groups)), dma((S,)), dma((S,)),
    ]
    inside, outside = pl.BlockSpec(memory_space=pltpu.VMEM), pl.BlockSpec(memory_space=pl.ANY)
    tile = 256 if ff % 256 == 0 else 128
    return pl.pallas_call(
        functools.partial(fused_kernel, (S, CW, groups, cap, stride, tile)),
        out_shape=jax.ShapeDtypeStruct((toks, width), BF16),
        in_specs=[inside] * 3 + [outside] * 3,
        out_specs=inside,
        scratch_shapes=scratch,
        compiler_params=pltpu.CompilerParams(collective_id=0, has_side_effects=True, vmem_limit_bytes=67043328),
    )(tokens, gain.reshape(1, width), meta, w_gate, w_up, w_down)


SPLIT = 4


def fits(mesh):
    return mesh.shape["mp"] == 8 and mesh.shape["expert"] <= 4


def solution(mesh):
    in_specs = (
        P(("expert", "mp"), None),
        P(),
        P(("expert", "mp"), None),
        P(("expert", "mp")),
        P("expert", None, "mp"),
        P("expert", None, "mp"),
        P("expert", "mp", None),
    )
    out_specs = P(("expert", "mp"), None)
    return jax.shard_map(fused_body if fits(mesh) else body, mesh=mesh, in_specs=in_specs, out_specs=out_specs, check_vma=False)
```

```python
import functools

import jax
import jax.numpy as jnp
from jax import lax
from jax.experimental import pallas as pl
from jax.experimental.pallas import tpu as pltpu
from jax.sharding import PartitionSpec as P

DENOM = 1024


def rms_normed(tokens, gain):
    values = tokens.astype(jnp.float32)
    inverse = lax.rsqrt(jnp.mean(values * values, axis=1, keepdims=True) + 1e-05)
    return (values * inverse * gain.astype(jnp.float32)).astype(jnp.bfloat16)


def swiglu(row_block, gate_matrix, up_matrix):
    gate_proj = jnp.dot(row_block, gate_matrix, preferred_element_type=jnp.float32)
    up_proj = jnp.dot(row_block, up_matrix, preferred_element_type=jnp.float32)
    return (jax.nn.silu(gate_proj) * up_proj).astype(jnp.bfloat16)


def slot_plan(expert_ids, experts, capacity):
    flat_ids = expert_ids.reshape(-1)
    slot_count = flat_ids.shape[0]
    slot_order = jnp.arange(slot_count, dtype=jnp.int32)
    earlier = (flat_ids[:, None] == flat_ids[None, :]) & (slot_order[None, :] < slot_order[:, None])
    position = jnp.sum(earlier.astype(jnp.int32), axis=1)
    target = flat_ids * capacity + position
    slot_ids = jnp.arange(experts * capacity, dtype=jnp.int32)
    matched = target[None, :] == slot_ids[:, None]
    token_of = slot_order[None, :] // expert_ids.shape[1] + 1
    slot_owner = jnp.sum(jnp.where(matched, token_of, 0), axis=1) - 1
    return (target, slot_owner)


def body(tokens, gain, expert_ids, gate_num, w_gate, w_up, w_down):
    groups = lax.axis_size("expert")
    tok_rows, model_width = tokens.shape
    top_count = expert_ids.shape[1]
    capacity = (5 * tok_rows * top_count + 4 * groups - 1) // (4 * groups)
    normed = rms_normed(tokens, gain)
    target, slot_owner = slot_plan(expert_ids, groups, capacity)
    gate_matrix = w_gate[0]
    up_matrix = w_up[0]
    down_matrix = w_down[0]
    picked = jnp.take(normed, jnp.maximum(slot_owner, 0), axis=0)
    outgoing = jnp.where((slot_owner >= 0)[:, None], picked, jnp.zeros_like(picked))
    received = lax.all_to_all(
        outgoing.reshape(groups, capacity, model_width),
        "expert",
        split_axis=0,
        concat_axis=0,
        tiled=True,
    )
    received = received.reshape(groups * capacity, model_width)
    hidden = swiglu(lax.all_gather(received, "mp", axis=0, tiled=True), gate_matrix, up_matrix)
    summed = lax.psum_scatter(
        jnp.dot(hidden, down_matrix, preferred_element_type=jnp.float32).astype(jnp.bfloat16),
        "mp",
        scatter_dimension=0,
        tiled=True,
    )
    outcome = summed.reshape(groups, capacity, model_width)
    returned = lax.all_to_all(outcome, "expert", split_axis=0, concat_axis=0, tiled=True)
    flat_back = returned.reshape(groups * capacity, model_width)
    chosen = (
        jnp.take(flat_back, target, axis=0)
        .astype(jnp.float32)
        .reshape(tok_rows, top_count, model_width)
    )
    first_share = gate_num.astype(jnp.float32) / DENOM
    mixed_out = (
        chosen[:, 0, :] * first_share[:, None] + chosen[:, 1, :] * (1.0 - first_share)[:, None]
    )
    return mixed_out.astype(jnp.bfloat16)


MESH = pl.DeviceIdType.MESH
F32, BF16 = jnp.float32, jnp.bfloat16


def fused_kernel(plan, tok_hbm, gain_hbm, ids_hbm, num_hbm, wg_hbm, wu_hbm, wd_hbm, out,
                 tok, gain, ids_loc, num_loc, ids_all, num_all, pad, i_sem, out_sem,
                 wg, wu, wd, xbuf, acc_g, acc_u, hidden, nbuf, norm_all,
                 zsend, zrecv, psend, prcv, sums, r1, s2, r2, rsend, zret, mixbuf, orecv,
                 w_sem, wd_sem, n_sem, m_sem, z_ss, z_rs, x_ss, x_rs, y_ss, y_rs, f_ss, f_rs,
                 d_ss, d_rs, p_ss, p_rs, a_ss, a_rs, b_ss, b_rs, q_ss, q_rs, o_ss, o_rs):
    S, CW, groups, cap, stride, tile = plan
    toks, width = tok.shape
    half = width // 2
    rows = groups * cap
    ff = hidden.shape[1]
    myz = lax.axis_index("expert")
    mp = lax.axis_index("mp")
    core = mp % 2
    other = 1 - core
    k = mp // 2
    kx = k + 1 - 2 * (k % 2)
    ky = k + 2 - 4 * (k // 2)
    kd = 3 - k
    partner = {"mp": 2 * k + other}
    xn = {"mp": 2 * kx + core}
    yn = {"mp": 2 * ky + core}
    zs = [lax.rem(myz + d, groups) for d in range(groups)]

    def remote(src, dst, ss, rs, dev):
        return pltpu.make_async_remote_copy(src_ref=src, dst_ref=dst, send_sem=ss, recv_sem=rs,
                                            device_id=dev, device_id_type=MESH)

    barrier = pltpu.get_barrier_semaphore()
    peers = [partner, xn, yn] + [{"expert": zs[d]} for d in range(1, groups)]
    for dev in peers:
        pl.semaphore_signal(barrier, inc=1, device_id=dev, device_id_type=MESH)

    order = []
    for j in range(S):
        order += [core * S + j, other * S + j]

    def w_copies(c):
        at = pl.ds(pl.multiple_of(c * CW, CW), CW)
        return (pltpu.make_async_copy(wg_hbm.at[0, at, :], wg.at[at, :], w_sem.at[0, c]),
                pltpu.make_async_copy(wu_hbm.at[0, at, :], wu.at[at, :], w_sem.at[1, c]))

    def wd_copy(c):
        at = pl.ds(pl.multiple_of(c * CW, CW), CW)
        return pltpu.make_async_copy(wd_hbm.at[0, :, at], wd.at[:, at], wd_sem.at[c])

    entries = [pltpu.make_async_copy(a, b, i_sem.at[i]) for i, (a, b) in enumerate(
        ((tok_hbm, tok), (gain_hbm, gain), (ids_hbm, ids_loc), (num_hbm, num_loc)))]
    for copy in entries:
        copy.start()

    pad[...] = jnp.zeros_like(pad)
    for copy in entries:
        copy.wait()
    for c in order:
        for copy in w_copies(c):
            copy.start()
    for j in range(S):
        wd_copy(other * S + j).start()
        wd_copy(core * S + j).start()
    ids_all[core] = ids_loc[...]
    num_all[core] = num_loc[...]
    values = tok[...].astype(F32)
    inverse = lax.rsqrt(jnp.mean(values * values, axis=1, keepdims=True) + 1e-05)
    gains = gain[...].astype(F32)
    for r in range(width // 128):
        part = values[:, r * 128:(r + 1) * 128] * inverse * gains[r:r + 1]
        at = r * 128 % half
        nbuf[r * 128 // half, :, at:at + 128] = part.astype(BF16)
    pl.semaphore_wait(barrier, len(peers))
    ids_copy = remote(ids_loc, ids_all.at[core], m_sem.at[0], m_sem.at[1], partner)
    num_copy = remote(num_loc, num_all.at[core], m_sem.at[2], m_sem.at[3], partner)
    ids_copy.start()
    num_copy.start()
    norm_copy = remote(nbuf.at[other], norm_all.at[core], n_sem.at[0], n_sem.at[1], partner)
    norm_copy.start()
    norm_all[core] = nbuf[core]

    ids_copy.wait_recv()
    num_copy.wait_recv()
    for c in range(2):
        pad[c, 0:2, 0:toks] = ids_all[c].astype(F32)
        pad[c, 2:3, 0:toks] = num_all[c].astype(F32)
    info = jnp.concatenate([jnp.transpose(pad[c])[:toks] for c in range(2)], axis=0).astype(jnp.int32)
    id0, id1, num = info[:, 0:1], info[:, 1:2], info[:, 2:3]
    lanes = lax.broadcasted_iota(jnp.int32, (2 * toks, 128), 1)
    oh0 = jnp.where(lanes == id0, 1.0, 0.0)
    oh1 = jnp.where(lanes == id1, 1.0, 0.0)
    tri_r = lax.broadcasted_iota(jnp.int32, (2 * toks, 2 * toks), 0)
    tri_c = lax.broadcasted_iota(jnp.int32, (2 * toks, 2 * toks), 1)
    tri = jnp.where(tri_c < tri_r, 1.0, 0.0).astype(BF16)
    cnt = jnp.dot(tri, (oh0 + oh1).astype(BF16), preferred_element_type=F32)
    lane_f = lanes.astype(F32)
    t0 = id0.astype(F32) * stride + jnp.sum(oh0 * cnt, axis=1, keepdims=True)
    t1 = id1.astype(F32) * stride + jnp.sum(oh1 * cnt, axis=1, keepdims=True)
    hit0, hit1 = lane_f == t0, lane_f == t1
    pick = jnp.where(hit0 | hit1, 1.0, 0.0)
    pick_t = jnp.transpose(pick).astype(BF16)
    low0 = num % 4
    low1 = (DENOM - num) % 4
    hi = jnp.where(hit0, (num - low0).astype(F32), jnp.where(hit1, (DENOM - num - low1).astype(F32), 0.0))
    lo = jnp.where(hit0, low0.astype(F32), jnp.where(hit1, low1.astype(F32), 0.0))
    mix = (jnp.concatenate([hi, lo], axis=0) * (1.0 / DENOM)).astype(BF16)

    norm_copy.wait_recv()

    def z_copy(j, d):
        return remote(zsend.at[j, zs[d]], zrecv.at[j, myz], z_ss.at[j, d], z_rs.at[j, d], {"expert": zs[d]})

    for j in range(S):
        block = norm_all[:, :, j * CW:(j + 1) * CW].reshape(2 * toks, CW)
        picked = jnp.dot(pick_t, block, preferred_element_type=F32).astype(BF16)
        for z in range(groups):
            zsend[j, z] = picked[z * stride:z * stride + cap]
        for d in range(1, groups):
            z_copy(j, d).start()
        zrecv[j, myz] = zsend[j, myz]

    acc_g[...] = jnp.zeros_like(acc_g)
    acc_u[...] = jnp.zeros_like(acc_u)

    def place(z):
        r = lax.broadcasted_iota(jnp.int32, (rows, cap), 0)
        c = lax.broadcasted_iota(jnp.int32, (rows, cap), 1)
        return jnp.where(r == c + z * cap, 1.0, 0.0).astype(BF16)

    def take(z):
        r = lax.broadcasted_iota(jnp.int32, (cap, rows), 0)
        c = lax.broadcasted_iota(jnp.int32, (cap, rows), 1)
        return jnp.where(c == r + z * cap, 1.0, 0.0).astype(BF16)

    def slot(j, who, core_of=core):
        return xbuf.at[core_of * S + j, who]

    def x_copy(j, who=None):
        return remote(slot(j, k), slot(j, k), x_ss.at[j], x_rs.at[j], xn)

    def y_copy(j):
        return remote(slot(j, k), slot(j, k), y_ss.at[j], y_rs.at[j], yn)

    def f_copy(j):
        if j % 2 == 0:
            return remote(slot(j, kx), slot(j, kx), f_ss.at[j], f_rs.at[j], yn)
        return remote(slot(j, ky), slot(j, ky), f_ss.at[j], f_rs.at[j], xn)

    whos = (k, kx, ky, kd)

    def d_copy(j, i):
        return remote(slot(j, whos[i]), slot(j, whos[i]), d_ss.at[j, i], d_rs.at[j, i], partner)

    def stage_c(j):
        total = jnp.zeros((rows, CW), F32)
        for d in range(1, groups):
            z_copy(j, d).wait_recv()
        for z in range(groups):
            total = total + jnp.dot(place(z), zrecv[j, z], preferred_element_type=F32)
        xbuf[core * S + j, k] = total.astype(BF16)
        x_copy(j).start()
        y_copy(j).start()
        d_copy(j, 0).start()

    def stage_d(j):
        x_copy(j).wait_recv()
        if j % 2 == 0:
            f_copy(j).start()
        d_copy(j, 1).start()
        y_copy(j).wait_recv()
        if j % 2 == 1:
            f_copy(j).start()
        d_copy(j, 2).start()

    def up_mm(c, last):
        for copy in w_copies(c):
            copy.wait()
        at = pl.ds(pl.multiple_of(c * CW, CW), CW)

        def step(n, carry):
            cols = pl.ds(pl.multiple_of(n * tile, tile), tile)
            x = xbuf[c].reshape(4 * rows, CW)
            g = acc_g[:, cols] + jnp.dot(x, wg[at, cols], preferred_element_type=F32)
            u = acc_u[:, cols] + jnp.dot(x, wu[at, cols], preferred_element_type=F32)
            if last:
                hidden[:, cols] = (g / (1.0 + jnp.exp(-g)) * u).astype(BF16)
            else:
                acc_g[:, cols] = g
                acc_u[:, cols] = u
            return carry

        lax.fori_loop(0, ff // tile, step, 0)

    def stage_e(j):
        stage_e1(j)
        stage_e2(j)

    def stage_e1(j):
        f_copy(j).wait_recv()
        d_copy(j, 3).start()
        up_mm(core * S + j, False)

    def stage_e2(j):
        for i in range(4):
            d_copy(j, i).wait_recv()
        up_mm(other * S + j, j == S - 1)

    stage_c(0)
    for j in range(1, S):
        stage_c(j)
        stage_d(j - 1)
        if j >= 2:
            stage_e(j - 2)
    stage_e1(S - 2)
    stage_d(S - 1)
    stage_e2(S - 2)
    stage_e(S - 1)

    def down(c):
        at = pl.ds(pl.multiple_of(c * CW, CW), CW)
        wd_copy(c).wait()
        return jnp.dot(hidden[...], wd[:, at], preferred_element_type=F32)

    def p_copy(j):
        return remote(psend.at[j], prcv.at[j], p_ss.at[j], p_rs.at[j], partner)

    def near(j):
        return (kx, ky, xn, yn) if j % 2 == 0 else (ky, kx, yn, xn)

    def a_copy(j, i):
        first, _, dev, _ = near(j)
        return remote(sums.at[j, (first, kd)[i]], r1.at[j, i], a_ss.at[j, i], a_rs.at[j, i], dev)

    def b_copy(j):
        return remote(s2.at[j], r2.at[j], b_ss.at[j], b_rs.at[j], near(j)[3])

    def stage_0a(j):
        psend[j] = down(other * S + j).astype(BF16).reshape(4, rows, CW)
        p_copy(j).start()

    def stage_0(j):
        own = down(core * S + j).reshape(4, rows, CW)
        p_copy(j).wait_recv()
        sums[j] = (own + prcv[j].astype(F32)).astype(BF16)

    def stage_1(j):
        a_copy(j, 1).start()
        a_copy(j, 0).start()

    def stage_2(j):
        a_copy(j, 1).wait_recv()
        s2[j] = (sums[j, near(j)[1]].astype(F32) + r1[j, 1].astype(F32)).astype(BF16)
        b_copy(j).start()

    def q_copy(j, d):
        return remote(rsend.at[j, zs[d]], zret.at[j, myz], q_ss.at[j, d], q_rs.at[j, d], {"expert": zs[d]})

    def stage_3(j):
        a_copy(j, 0).wait_recv()
        b_copy(j).wait_recv()
        fin = (sums[j, k].astype(F32) + r1[j, 0].astype(F32) + r2[j].astype(F32)).astype(BF16)
        for z in range(groups):
            rsend[j, z] = jnp.dot(take(z), fin, preferred_element_type=F32).astype(BF16)
        for d in range(1, groups):
            q_copy(j, d).start()
        zret[j, myz] = rsend[j, myz]

    def o_copy(j):
        return remote(mixbuf.at[j, other], orecv.at[j], o_ss.at[j], o_rs.at[j], partner)

    def stage_4(j):
        for d in range(1, groups):
            q_copy(j, d).wait_recv()
        total = jnp.zeros((4 * toks, CW), F32)
        for z in range(groups):
            total = total + jnp.dot(mix[:, z * stride:z * stride + cap], zret[j, z], preferred_element_type=F32)
        mixed = (total[:2 * toks] + total[2 * toks:]).astype(BF16)
        mixbuf[j] = mixed.reshape(2, toks, CW)
        o_copy(j).start()
        out_copy(j, 0).start()

    def out_copy(j, i):
        cols = pl.ds(pl.multiple_of(((core, other)[i] * S + j) * CW, CW), CW)
        return pltpu.make_async_copy((mixbuf.at[j, core], orecv.at[j])[i], out.at[:, cols], out_sem.at[j, i])

    stage_0a(0)
    for j in range(S):
        if j + 1 < S:
            stage_0a(j + 1)
        stage_0(j)
        if j < 2:
            stage_1(j)
    for j in range(0, S, 2):
        stage_2(j)
        stage_2(j + 1)
        if j + 2 < S:
            stage_1(j + 2)
            stage_1(j + 3)
        stage_3(j)
        stage_3(j + 1)
    for j in range(S):
        stage_4(j)
    for j in range(S):
        o_copy(j).wait_recv()
        out_copy(j, 1).start()

    ids_copy.wait_send()
    num_copy.wait_send()
    norm_copy.wait_send()
    for j in range(S):
        for d in range(1, groups):
            z_copy(j, d).wait_send()
            q_copy(j, d).wait_send()
        for copy in (x_copy(j), y_copy(j), f_copy(j), p_copy(j), a_copy(j, 0), a_copy(j, 1), b_copy(j), o_copy(j)):
            copy.wait_send()
        for i in range(4):
            d_copy(j, i).wait_send()
        out_copy(j, 0).wait()
        out_copy(j, 1).wait()


def fused_body(tokens, gain, expert_ids, gate_num, w_gate, w_up, w_down):
    groups = lax.axis_size("expert")
    toks, width = tokens.shape
    ff = w_gate.shape[2]
    cap = 2 * ((5 * toks * expert_ids.shape[1] + 4 * groups - 1) // (4 * groups))
    stride = -(-cap // 16) * 16
    rows = groups * cap
    S = SPLIT
    CW = width // 2 // S
    dma = pltpu.SemaphoreType.DMA
    vm = pltpu.VMEM
    scratch = [
        vm((toks, width), BF16), vm((width // 128, 128), BF16), vm((2, toks), jnp.int32), vm((1, toks), jnp.int32),
        vm((2, 2, toks), jnp.int32), vm((2, 1, toks), jnp.int32), vm((2, 8, 128), F32), dma((4,)), dma((S, 2)),
        vm((width, ff), BF16), vm((width, ff), BF16), vm((ff, width), BF16),
        vm((2 * S, 4, rows, CW), BF16), vm((4 * rows, ff), F32), vm((4 * rows, ff), F32), vm((4 * rows, ff), BF16),
        vm((2, toks, width // 2), BF16), vm((2, toks, width // 2), BF16),
        vm((S, groups, cap, CW), BF16), vm((S, groups, cap, CW), BF16),
        vm((S, 4, rows, CW), BF16), vm((S, 4, rows, CW), BF16), vm((S, 4, rows, CW), BF16),
        vm((S, 2, rows, CW), BF16), vm((S, rows, CW), BF16), vm((S, rows, CW), BF16),
        vm((S, groups, cap, CW), BF16), vm((S, groups, cap, CW), BF16),
        vm((S, 2, toks, CW), BF16), vm((S, toks, CW), BF16),
        dma((2, 2 * S)), dma((2 * S,)), dma((2,)), dma((4,)),
        dma((S, groups)), dma((S, groups)), dma((S,)), dma((S,)), dma((S,)), dma((S,)), dma((S,)), dma((S,)),
        dma((S, 4)), dma((S, 4)), dma((S,)), dma((S,)), dma((S, 2)), dma((S, 2)), dma((S,)), dma((S,)),
        dma((S, groups)), dma((S, groups)), dma((S,)), dma((S,)),
    ]
    outside = pl.BlockSpec(memory_space=pl.ANY)
    tile = 256 if ff % 256 == 0 else 128
    return pl.pallas_call(
        functools.partial(fused_kernel, (S, CW, groups, cap, stride, tile)),
        out_shape=jax.ShapeDtypeStruct((toks, width), BF16),
        in_specs=[outside] * 7,
        out_specs=outside,
        scratch_shapes=scratch,
        compiler_params=pltpu.CompilerParams(collective_id=0, has_side_effects=True, vmem_limit_bytes=67043328),
    )(tokens, gain.reshape(width // 128, 128), expert_ids.T, gate_num.reshape(1, toks), w_gate, w_up, w_down)


SPLIT = 4


def fits(mesh):
    return mesh.shape["mp"] == 8 and mesh.shape["expert"] <= 4


def solution(mesh):
    in_specs = (
        P(("expert", "mp"), None),
        P(),
        P(("expert", "mp"), None),
        P(("expert", "mp")),
        P("expert", None, "mp"),
        P("expert", None, "mp"),
        P("expert", "mp", None),
    )
    out_specs = P(("expert", "mp"), None)
    return jax.shard_map(fused_body if fits(mesh) else body, mesh=mesh, in_specs=in_specs, out_specs=out_specs, check_vma=False)
```
